32 devices in a mesh: dp: 8 (over y, x, core), head: 4 (over z).
Axes of the slice: x: 2, y: 2, z: 4, core: 2. Of those that a mesh axis runs over, the one named last changes fastest.
Arguments:
- attn_queries: bfloat16 [4096, 1536], P('dp', 'head'), may hold values from -64 to 64
- keys: bfloat16 [4096, 256], P('dp'), may hold values from -6 to 6
- values: bfloat16 [4096, 256], P('dp'), may hold values from -6 to 6
- out_weight: bfloat16 [1536, 1536], P('head'), may hold values from -0.15625 to 0.15625
- lengths: int32 [8, 8], P('dp'), may hold values from 1 to 256, 512 in all within a row
- queries: bfloat16 [32, 1536], P('dp', 'head'), may hold values from -48 to 48
- positives: int32 [32], replicated, may hold values from 0 to 63
Outputs:
- d_values: bfloat16 [4096, 256], P('dp', 'head')
- loss: float32 [], replicated
The draws below stay inside these ranges and needn't reach their ends.
Inputs may be any that keep to these rules, and one draw needn't show every extreme that they name: `lengths`: each row sums to 512.
All inputs are finite; a program needn't handle non-finite values.
Results may differ from the reference program's by a relative error of at most 0.0072.
Values may be sent and summed in bfloat16 or wider, within the bound.
A program may use at most 64 MiB of HBM per device.

```python
import math
import jax
import jax.numpy as jnp
import numpy as np
from jax import lax

D = 1536
HEADS = 12
KV_HEADS = 2
HD = 128
TOK_DEV = 512
DOCS_DEV = 8
NDOC = 64
NQ = 32
TOKENS = 4096
N_DP = 8


def draw_attn_queries(key, part):
    base_key = jax.random.fold_in(key, 11)
    normal = jnp.clip(jax.random.normal(base_key, (TOKENS, HEADS * HD), jnp.float32), -4.0, 4.0)
    return normal.astype(jnp.bfloat16)


def draw_queries(key, part):
    base_key = jax.random.fold_in(key, 21)
    normal = jnp.clip(jax.random.normal(base_key, (NQ, D), jnp.float32), -4.0, 4.0) / jnp.sqrt(1.0 * D)
    return normal.astype(jnp.bfloat16)


def with_ends(values, key, least, top_value):
    longest = values.shape.index(max(values.shape))
    spots = []
    for shift in (0, 1):
        where = [jax.random.randint(jax.random.fold_in(key, axis), (), 0, length) for axis, length in enumerate(values.shape)]
        where[longest] = (where[longest] + shift) % values.shape[longest]
        spots.append(tuple(where))
    return values.at[spots[0]].set(least).at[spots[1]].set(top_value)


def steps_of(key, extent, shards, smallest, high):
    factor_of = 1.0
    for position, parts in shards:
        steps = jax.random.uniform(jax.random.fold_in(jax.random.fold_in(key, 6), position), (parts,), jnp.float32, smallest / len(shards), high / len(shards))
        factor_of = factor_of * jnp.repeat(jnp.exp(steps), extent[position] // parts).reshape((-1,) + (1,) * (len(extent) - 1 - position))
    return factor_of


def profile(count, total, bound, skew):
    loads = [(1 << 20) // math.isqrt(grade ** skew) + 1 for grade in range(2, count + 1)]
    spare, holding = total - bound - (count - 1), [1] * (count - 1)
    while spare > 0:
        free = [i for i in range(count - 1) if holding[i] < bound]
        mass, left = sum([loads[i] for i in free]), spare
        for i in free:
            extra = min(bound - holding[i], max(1, left * loads[i] // mass), spare)
            holding[i] = holding[i] + extra
            spare = spare - extra
    return np.array([bound] + holding)


def uneven(stream_key, amount, total, most, lean):
    if amount == 2:
        one = jax.random.randint(stream_key, (), max(1, total - most), min(most, total - 1) + 1)
        return jnp.stack([one, total - one])
    sizes = jnp.asarray(profile(amount, total, most, lean), jnp.int32)
    couples = (amount - 1) // 2
    giver, taker = sizes[1:1 + 2 * couples:2], sizes[2:2 + 2 * couples:2]
    slack = jnp.minimum(giver - 1, most - taker)
    shifted = jax.random.randint(jax.random.fold_in(stream_key, 1), (couples,), 0, 1 << 20) % (slack + 1)
    sizes = sizes.at[1:1 + 2 * couples:2].set(giver - shifted).at[2:2 + 2 * couples:2].set(taker + shifted)
    return sizes[jax.random.permutation(jax.random.fold_in(stream_key, 2), amount)]


def normal_values(own_key, extent, deviation, most, pieces=(), held_as=jnp.bfloat16):
    values = jax.random.normal(own_key, extent, jnp.float32) * deviation
    if len(pieces) > 0:
        values = steps_of(own_key, extent, pieces, -0.22, 0.18) * values
    return jnp.clip(values, min=-most, max=most).astype(held_as)


def setup_inputs(seed: int = 0) -> dict:
    streams_of = jax.random.split(jax.random.key(seed), 8)
    attn_queries = draw_attn_queries(jax.random.fold_in(streams_of[7], 71), 0)
    keys = normal_values(streams_of[1], (TOKENS, KV_HEADS * HD), 1.0, 6.0, ((0, 8),))
    values = normal_values(streams_of[2], (TOKENS, KV_HEADS * HD), 1.0, 6.0, ((0, 8),))
    out_weight = normal_values(streams_of[3], (HEADS * HD, D), (HEADS * HD) ** -0.5, 0.15625, ((0, 4),))
    lengths = jax.vmap(lambda own: uneven(own, DOCS_DEV, TOK_DEV, TOK_DEV // 2, 2))(jax.random.split(streams_of[4], N_DP)).reshape((N_DP, DOCS_DEV)).astype(jnp.int32)
    queries = draw_queries(jax.random.fold_in(streams_of[7], 71), 0)
    positives = with_ends(jax.random.randint(streams_of[6], (NQ,), 0, NDOC), jax.random.fold_in(streams_of[6], 1), 0, NDOC - 1).astype(jnp.int32)
    return dict(attn_queries=attn_queries, keys=keys, values=values, out_weight=out_weight, lengths=lengths, queries=queries, positives=positives)


sim_scale = 20.0
loss_scale = 32768.0

def segment_ids(lens):
    ends = jnp.cumsum(lens)
    places = jnp.arange(TOK_DEV, dtype=jnp.int32)
    return lax.optimization_barrier(jnp.sum((places[:, None] >= ends[None, :]).astype(jnp.int32), axis=1))

def attend_probs(queries_h, keys_h, seg):
    scores = jnp.einsum('hqd,hkd->hqk', queries_h, keys_h, precision=lax.Precision.HIGHEST) / math.sqrt(HD)
    places = jnp.arange(TOK_DEV, dtype=jnp.int32)
    allowed = (seg[:, None] == seg[None, :]) & (places[None, :] <= places[:, None])
    scores = jnp.where(allowed[None], scores, -1e+30)
    top = lax.optimization_barrier(jnp.max(scores, axis=-1, keepdims=True))
    expo = jnp.exp(scores - top)
    return (expo / lax.optimization_barrier(jnp.sum(expo, axis=-1, keepdims=True))).astype(jnp.bfloat16)

def reference(attn_queries, keys, values, out_weight, lengths, queries, positives):
    width = HEADS * HD
    group = HEADS // KV_HEADS
    owner = jnp.arange(HEADS, dtype=jnp.int32) // group

    def split(array, index, count):
        piece = lax.dynamic_slice_in_dim(array, index * TOK_DEV, TOK_DEV, 0)
        return piece.reshape(TOK_DEV, count, HD).transpose(1, 0, 2).astype(jnp.float32)

    def member_of(seg):
        return jnp.arange(DOCS_DEV, dtype=jnp.int32)[:, None] == seg[None, :]

    def probs_of(index, seg):
        keys_all = split(keys, index, KV_HEADS)[owner]
        return attend_probs(split(attn_queries, index, HEADS), keys_all, seg)

    def forward(index):
        seg = segment_ids(lengths[index])
        probs = probs_of(index, seg)
        values_all = split(values, index, KV_HEADS)[owner]
        context = jnp.einsum('hqk,hkd->hqd', probs.astype(jnp.float32), values_all, precision=lax.Precision.HIGHEST)
        context = context.astype(jnp.bfloat16).transpose(1, 0, 2).reshape(TOK_DEV, width)
        sums = jnp.dot(member_of(seg).astype(jnp.bfloat16), context, preferred_element_type=jnp.float32)
        return sums / lengths[index][:, None].astype(jnp.float32)
    seq_index = jnp.arange(N_DP, dtype=jnp.int32)
    pooled = lax.map(forward, seq_index).reshape(N_DP * DOCS_DEV, width)
    weight = out_weight.astype(jnp.float32)
    emb = jnp.dot(pooled, weight, precision=lax.Precision.HIGHEST)
    rnorm = 1.0 / jnp.sqrt(lax.optimization_barrier(jnp.sum(emb * emb, axis=1)) + 1e-06)
    unit = emb * rnorm[:, None]
    unit_b = unit.astype(jnp.bfloat16)
    logits = sim_scale * jnp.dot(queries, unit_b.T, preferred_element_type=jnp.float32)
    top = lax.optimization_barrier(jnp.max(logits, axis=1))
    lse = top + jnp.log(lax.optimization_barrier(jnp.sum(jnp.exp(logits - top[:, None]), axis=1)))
    chosen = (jnp.arange(N_DP * DOCS_DEV, dtype=jnp.int32)[None, :] == positives[:, None]).astype(jnp.float32)
    pos_logit = lax.optimization_barrier(jnp.sum(logits * chosen, axis=1))
    loss = jnp.mean(lse - pos_logit)
    dlogits = jnp.exp(logits - lse[:, None]) - chosen
    g_unit = sim_scale * jnp.dot(dlogits.T, queries.astype(jnp.float32), precision=lax.Precision.HIGHEST)
    inner = lax.optimization_barrier(jnp.sum(unit * g_unit, axis=1))
    g_emb = rnorm[:, None] * (g_unit - unit * inner[:, None])
    g_pooled = jnp.dot(g_emb, weight.T, precision=lax.Precision.HIGHEST)

    def backward(index):
        seg = segment_ids(lengths[index])
        probs = probs_of(index, seg)
        rows = lax.dynamic_slice_in_dim(g_pooled, index * DOCS_DEV, DOCS_DEV, 0)
        scaled = rows / lengths[index][:, None].astype(jnp.float32) * loss_scale
        d_context = jnp.dot(member_of(seg).astype(jnp.float32).T, scaled, precision=lax.Precision.HIGHEST)
        d_context = d_context.astype(jnp.bfloat16).reshape(TOK_DEV, HEADS, HD).transpose(1, 0, 2).astype(jnp.float32)
        grads = jnp.einsum('hqk,hqd->hkd', probs.astype(jnp.float32), d_context, precision=lax.Precision.HIGHEST)
        grads = lax.optimization_barrier(jnp.sum(grads.reshape(KV_HEADS, group, TOK_DEV, HD), axis=1))
        return grads.astype(jnp.bfloat16).transpose(1, 0, 2).reshape(TOK_DEV, KV_HEADS * HD)
    d_values = lax.map(backward, seq_index).reshape(N_DP * TOK_DEV, KV_HEADS * HD)
    return (d_values, loss)
```

```python
import functools
import math

import jax
import jax.numpy as jnp
from jax import lax
from jax.experimental import pallas as pl
from jax.experimental.pallas import tpu as pltpu
from jax.sharding import PartitionSpec as P

HEADS = 12
KV_HEADS = 2
HD = 128
LANES = 128
SUBLANES = 8

sim_scale = 20.0
loss_scale = 32768.0

NT = (((1,), (1,)), ((), ()))
NN = (((1,), (0,)), ((), ()))
f32 = jnp.float32
bf16 = jnp.bfloat16


def mm(a, b, dims):
    return lax.dot_general(a, b, dims, preferred_element_type=f32)


def hi_lo(x):
    hi = x.astype(bf16)
    return hi, (x - hi.astype(f32)).astype(bf16)


def each(first, last, body):
    if last - first <= 8:
        for k in range(first, last):
            body(k)
    else:
        lax.fori_loop(first, last, lambda k, c: (body(k), c)[1], 0)


def fold(last, body, carry):
    if last <= 8:
        for k in range(last):
            carry = body(k, carry)
        return carry
    return lax.fori_loop(0, last, body, carry)


def remote(src, dst, send, recv, axis, peer):
    return pltpu.make_async_remote_copy(
        src_ref=src, dst_ref=dst, send_sem=send, recv_sem=recv,
        device_id={axis: peer}, device_id_type=pl.DeviceIdType.MESH,
    )


def wait_all(ref, sem):
    pltpu.make_async_copy(ref, ref, sem).wait()


def kernel(
    n_dp, n_head,
    lens_hbm, pos_hbm, q_hbm, k_hbm, v_hbm, w_hbm, qry_hbm,
    out_ref, loss_ref,
    lens, pos_ref, q_v, k_v, v_v, w_v, qall, qf, c_own, c_in, emb_slot, stat, qw_own, qw_in, uw_own, uw_in,
    a_ref, load_sem, qload_sem, q1_send, q1_recv, q2_send, q2_recv, e_send, e_recv, s_send, s_recv,
    p_send, p_recv,
):
    dp = lax.axis_index("dp")
    head = lax.axis_index("head")
    side = lax.rem(head, 2)
    partner = head + 1 - 2 * side
    seq, width = q_v.shape
    heads = width // HD
    half = HD // 2
    group = HEADS // KV_HEADS
    docs = lens.shape[1]
    rows = qall.shape[2]
    nq = n_dp * rows
    kv_cols = pl.ds(pl.multiple_of((head * heads // group) * HD, HD), HD)
    blocks = seq // LANES

    k_load = pltpu.make_async_copy(k_hbm.at[:, kv_cols], k_v, load_sem.at[0])
    v_load = pltpu.make_async_copy(v_hbm.at[:, kv_cols], v_v, load_sem.at[1])
    w_load = pltpu.make_async_copy(w_hbm, w_v, load_sem.at[2])
    qry_load = pltpu.make_async_copy(qry_hbm, qall.at[dp, head], load_sem.at[3])
    q_loads = [
        pltpu.make_async_copy(
            q_hbm.at[pl.ds(b * LANES, LANES)], q_v.at[pl.ds(b * LANES, LANES)], qload_sem.at[b]
        )
        for b in range(blocks)
    ]
    lens_load = pltpu.make_async_copy(lens_hbm, lens, load_sem.at[4])
    pos_load = pltpu.make_async_copy(pos_hbm, pos_ref, load_sem.at[5])
    lens_load.start()
    k_load.start()
    q_loads[0].start()
    qry_load.start()
    for load in q_loads[1:]:
        load.start()
    v_load.start()
    w_load.start()
    pos_load.start()

    barrier = pltpu.get_barrier_semaphore()

    def peer(me, k, n):
        return lax.bitwise_xor(me, n - k)

    def greet(axis, me, n):
        def one(k):
            pl.semaphore_signal(
                barrier, inc=1, device_id={axis: peer(me, k, n)}, device_id_type=pl.DeviceIdType.MESH
            )
        each(1, n, one)

    greet("head", head, n_head)
    greet("dp", dp, n_dp)

    def q1(k, owner):
        slot = qall.at[dp, owner]
        return remote(slot, slot, q1_send, q1_recv.at[k], "head", peer(head, k, n_head))

    def q2(x, k, owner):
        slot = qall.at[owner, lax.bitwise_xor(head, x)]
        return remote(slot, slot, q2_send, q2_recv.at[x], "dp", peer(dp, k, n_dp))

    def e_copy(k, owner):
        slot = emb_slot.at[owner]
        return remote(slot, slot, e_send, e_recv, "head", peer(head, k, n_head))

    def s_copy(k, owner):
        slot = stat.at[owner]
        return remote(slot, slot, s_send, s_recv, "dp", peer(dp, k, n_dp))

    ii = lax.broadcasted_iota(jnp.int32, (1, seq), 1)
    drow = lax.broadcasted_iota(jnp.int32, (docs, 1), 0)
    start_row = jnp.zeros((1, seq), jnp.int32)
    starts = jnp.zeros((docs, 1), jnp.int32)
    lens_col = jnp.zeros((docs, 1), jnp.int32)
    begin = jnp.int32(0)
    lens_load.wait()
    for d in range(docs):
        start_row = jnp.where(ii >= begin, begin, start_row)
        starts = jnp.where(drow == d, begin, starts)
        lens_col = jnp.where(drow == d, lens[0, d], lens_col)
        begin = begin + lens[0, d]
    len_f = lens_col.astype(f32)
    member = (ii >= starts) & (ii < starts + lens_col)

    k_load.wait()
    ones = jnp.ones((docs, LANES), bf16)
    rate = math.log2(math.e) / math.sqrt(HD)
    sums = [[None] * blocks for _ in range(heads)]
    for b in range(blocks):
        q_loads[b].wait()
        n = (b + 1) * LANES
        cols = slice(b * LANES, n)
        jj = lax.broadcasted_iota(jnp.int32, (n, LANES), 0)
        allowed = (jj >= start_row[:, cols]) & (jj <= ii[:, cols])
        keys = k_v[:n, :]
        for h in range(heads):
            s = mm(keys, q_v[cols, h * HD:(h + 1) * HD], NT)
            s = jnp.where(allowed, s, -1e30)
            e = jnp.exp2((s - jnp.max(s, axis=0, keepdims=True)) * rate)
            p = (e * (1.0 / jnp.sum(e, axis=0, keepdims=True))).astype(bf16)
            part = mm(ones, p, NT)
            for j in range(b + 1):
                piece = part[:, j * LANES:(j + 1) * LANES]
                sums[h][j] = piece if sums[h][j] is None else sums[h][j] + piece
        if b == 1:
            qry_load.wait()
            pl.semaphore_wait(barrier, n_head - 1 + n_dp - 1)
            each(1, n_head, lambda k: q1(k, head).start())
            each(1, n_dp, lambda k: q2(0, k, dp).start())

    csum = [jnp.concatenate(sums[h], axis=1) for h in range(heads)]
    spread = jnp.concatenate([jnp.where(member, csum[h], 0.0) for h in range(heads)], axis=0)
    s_hi, s_lo = hi_lo(spread)
    v_load.wait()
    span = heads * docs
    pooled = mm(jnp.concatenate([s_hi, s_lo], axis=0), v_v[...], NN)
    pooled = pooled[:span] + pooled[span:]
    pooled = jnp.concatenate(
        [pooled[h * docs:(h + 1) * docs] for h in range(heads)], axis=1
    ) / len_f
    p_hi, p_lo = hi_lo(pooled)
    w_load.wait()
    emb = mm(jnp.concatenate([p_hi, p_lo], axis=0), w_v[...], NN)
    emb_slot[head] = (emb[:docs] + emb[docs:]).astype(bf16)
    each(1, n_head, lambda k: e_copy(k, head).start())

    rid = lax.broadcasted_iota(jnp.int32, (c_own.shape[0], 1), 0)
    packed = jnp.zeros(c_own.shape, f32)
    for h in range(heads):
        packed = jnp.where(rid == h, csum[h][:c_own.shape[0]], packed)
    c_own[...] = packed
    c_copy = remote(c_own, c_in, p_send.at[0], p_recv.at[0], "head", partner)
    c_copy.start()
    for x in range(1, n_head):
        q1(n_head - x, lax.bitwise_xor(head, x)).wait_recv()
        each(1, n_dp, lambda k: q2(x, k, dp).start())

    for x in range(n_head):
        wait_all(qall.at[pl.ds(0, n_dp - 1), 0], q2_recv.at[x])
    pack = max(1, SUBLANES // rows)

    def assemble(t):
        for o in range(n_head):
            piece = jnp.concatenate([qall[t * pack + u, o].astype(f32) for u in range(pack)], axis=0)
            qf[pl.ds(t * pack * rows, pack * rows), o * width:(o + 1) * width] = piece

    each(0, n_dp // pack, assemble)
    qmat = qf[...].astype(bf16)

    def w_half(which):
        return jnp.concatenate(
            [w_v[pl.ds(pl.multiple_of(h * HD + which * half, half), half), :] for h in range(heads)], axis=0
        )

    qw_own[...] = mm(qmat, w_half(1 - side), NT).astype(bf16)
    qw_copy = remote(qw_own, qw_in, p_send.at[1], p_recv.at[1], "head", partner)
    qw_copy.start()
    qw_mine = mm(qmat, w_half(side), NT).astype(bf16)

    c_copy.wait_recv()
    other = jnp.concatenate(
        [jnp.where(member, c_in[h:h + 1, :], 0.0) for h in range(heads)], axis=0
    )
    both = jnp.concatenate([spread, other], axis=0)
    b_hi, b_lo = hi_lo(both)
    a_ref[...] = jnp.concatenate([b_hi, b_lo], axis=0)
    qw_copy.wait_recv()
    qw = jnp.concatenate([qw_mine, qw_in[...]], axis=1)
    qw2 = jnp.concatenate([qw, qw], axis=0)
    pos_load.wait()
    chosen = (pos_ref[...] == dp * docs + drow).astype(f32)

    wait_all(emb_slot.at[pl.ds(0, n_head - 1)], e_recv)
    emb = emb_slot[0].astype(f32)
    for o in range(1, n_head):
        emb = emb + emb_slot[o].astype(f32)
    rnorm = 1.0 / jnp.sqrt(jnp.sum(emb * emb, axis=1, keepdims=True) + 1e-06)
    unit = emb * rnorm
    u_hi, u_lo = hi_lo(unit)
    u_both = jnp.concatenate([u_hi, u_lo], axis=0)
    sims = sim_scale * mm(u_both, qmat, NT)
    logits = sims[:docs]
    full = logits + sims[docs:]
    top = jnp.max(logits, axis=0, keepdims=True)
    total = jnp.sum(jnp.exp(logits - top), axis=0, keepdims=True)
    hit = jnp.sum(logits * chosen, axis=0, keepdims=True)
    srow = lax.broadcasted_iota(jnp.int32, (stat.shape[1], 1), 0)
    stat[dp] = jnp.where(srow == 0, top, jnp.where(srow == 1, total, hit))
    each(1, n_dp, lambda k: s_copy(k, dp).start())

    uw = mm(u_both, w_half(1 - side), NT)
    uw_own[...] = uw[:docs] + uw[docs:]
    uw_copy = remote(uw_own, uw_in, p_send.at[2], p_recv.at[2], "head", partner)
    uw_copy.start()
    uw = mm(u_both, w_half(side), NT)
    uw = uw[:docs] + uw[docs:]
    factor = rnorm * (loss_scale / len_f)

    wait_all(stat.at[pl.ds(0, n_dp - 1)], s_recv)
    top = fold(
        n_dp, lambda k, c: jnp.maximum(c, stat[k][0:1]), jnp.full((1, nq), -jnp.inf, f32)
    )

    def gather(k, c):
        tile = stat[k]
        return c[0] + tile[1:2] * jnp.exp(tile[0:1] - top), c[1] + tile[2:3]

    zero = jnp.zeros((1, nq), f32)
    total, hit = fold(n_dp, gather, (zero, zero))
    lse = top + jnp.log(total)
    loss_ref[0, 0] = jnp.sum(lse - hit) * (1.0 / nq)
    dl = jnp.exp(logits - lse) - chosen
    inner = jnp.sum(dl * full, axis=1, keepdims=True)
    d_hi, d_lo = hi_lo(dl)
    g = sim_scale * mm(jnp.concatenate([d_hi, d_lo], axis=1), qw2, NN)
    uw_copy.wait_recv()
    uw2 = jnp.concatenate([uw, uw_in[...]], axis=1)
    g = factor * (g - inner * uw2)
    small = jnp.concatenate(
        [g[:, h * half:(h + 1) * half] for h in range(2 * heads)], axis=0
    )
    small = jnp.concatenate([small, small], axis=0).T.astype(bf16)
    out_ref[...] = mm(small, a_ref[...], NN).astype(bf16)

    wait_all(qall.at[0, pl.ds(0, n_head - 1)], q1_send)
    wait_all(qall.at[pl.ds(0, n_dp - 1)], q2_send)
    wait_all(emb_slot.at[pl.ds(0, n_head - 1)], e_send)
    wait_all(stat.at[pl.ds(0, n_dp - 1)], s_send)
    c_copy.wait_send()
    qw_copy.wait_send()
    uw_copy.wait_send()


def store(x_ref, l_ref, o_ref, lo_ref, sem):
    copies = [
        pltpu.make_async_copy(x_ref, o_ref, sem.at[0]),
        pltpu.make_async_copy(l_ref, lo_ref, sem.at[1]),
    ]
    for copy in copies:
        copy.start()
    for copy in copies:
        copy.wait()


def per_device(n_dp, n_head, attn_queries, keys, values, out_weight, lengths, queries, positives):
    seq, width = attn_queries.shape
    heads = width // HD
    docs = lengths.shape[1]
    rows = queries.shape[0]
    nq = n_dp * rows
    model = out_weight.shape[1]
    blocks = seq // LANES
    half = width // 2
    dma = pltpu.SemaphoreType.DMA
    hbm = pl.BlockSpec(memory_space=pltpu.HBM)
    vmem = pl.BlockSpec(memory_space=pltpu.VMEM)
    smem = pl.BlockSpec(memory_space=pltpu.SMEM)
    d_values, loss = pl.pallas_call(
        functools.partial(kernel, n_dp, n_head),
        out_shape=(
            pltpu.VMEM((HD // 2, seq), bf16),
            pltpu.SMEM((1, 1), f32),
        ),
        in_specs=[hbm, hbm, hbm, hbm, hbm, hbm, hbm],
        out_specs=(vmem, smem),
        scratch_shapes=[
            pltpu.SMEM((1, docs), jnp.int32),
            pltpu.VMEM((1, nq), jnp.int32),
            pltpu.VMEM((seq, width), bf16),
            pltpu.VMEM((seq, HD), bf16),
            pltpu.VMEM((seq, HD), bf16),
            pltpu.VMEM((width, model), bf16),
            pltpu.VMEM((n_dp, n_head, rows, width), bf16),
            pltpu.VMEM((nq, model), f32),
            pltpu.VMEM((SUBLANES // 2, seq), f32),
            pltpu.VMEM((SUBLANES // 2, seq), f32),
            pltpu.VMEM((n_head, docs, model), bf16),
            pltpu.VMEM((n_dp, SUBLANES // 2, nq), f32),
            pltpu.VMEM((nq, half), bf16),
            pltpu.VMEM((nq, half), bf16),
            pltpu.VMEM((docs, half), f32),
            pltpu.VMEM((docs, half), f32),
            pltpu.VMEM((4 * heads * docs, seq), bf16),
            dma((6,)),
            dma((blocks,)),
            dma,
            dma((n_head,)),
            dma,
            dma((n_head,)),
            dma,
            dma,
            dma,
            dma,
            dma((3,)),
            dma((3,)),
        ],
        compiler_params=pltpu.CompilerParams(collective_id=0, has_side_effects=True),
    )(lengths, positives.reshape(1, nq), attn_queries, keys, values, out_weight, queries)
    d_values = pltpu.with_memory_space_constraint(d_values, pltpu.VMEM)
    loss = pltpu.with_memory_space_constraint(loss, pltpu.SMEM)
    d_values, loss = pl.pallas_call(
        store,
        out_shape=(
            jax.ShapeDtypeStruct((HD // 2, seq), bf16),
            jax.ShapeDtypeStruct((1, 1), f32),
        ),
        in_specs=[vmem, smem],
        out_specs=(hbm, hbm),
        scratch_shapes=[dma((2,))],
    )(d_values, loss)
    return d_values.T, loss.reshape(())


def solution(mesh):
    placed = (
        P("dp", "head"),
        P("dp", None),
        P("dp", None),
        P("head", None),
        P("dp", None),
        P("dp", "head"),
        P(),
    )
    return jax.shard_map(
        functools.partial(per_device, mesh.shape["dp"], mesh.shape["head"]),
        mesh=mesh, in_specs=placed, out_specs=(P("dp", "head"), P()), check_vma=False,
    )
```

```python
import functools
import math

import jax
import jax.numpy as jnp
from jax import lax
from jax.experimental import pallas as pl
from jax.experimental.pallas import tpu as pltpu
from jax.sharding import PartitionSpec as P

HEADS = 12
KV_HEADS = 2
HD = 128
LANES = 128
SUBLANES = 8
LONGEST = 256

sim_scale = 20.0
loss_scale = 32768.0

NT = (((1,), (1,)), ((), ()))
NN = (((1,), (0,)), ((), ()))
f32 = jnp.float32
bf16 = jnp.bfloat16


def mm(a, b, dims):
    return lax.dot_general(a, b, dims, preferred_element_type=f32)


def hi_lo(x):
    hi = x.astype(bf16)
    return hi, (x - hi.astype(f32)).astype(bf16)


def each(first, last, body):
    if last - first <= 8:
        for k in range(first, last):
            body(k)
    else:
        lax.fori_loop(first, last, lambda k, c: (body(k), c)[1], 0)


def fold(last, body, carry):
    if last <= 8:
        for k in range(last):
            carry = body(k, carry)
        return carry
    return lax.fori_loop(0, last, body, carry)


def remote(src, dst, send, recv, axis, peer):
    return pltpu.make_async_remote_copy(
        src_ref=src, dst_ref=dst, send_sem=send, recv_sem=recv,
        device_id={axis: peer}, device_id_type=pl.DeviceIdType.MESH,
    )


def wait_all(ref, sem):
    pltpu.make_async_copy(ref, ref, sem).wait()


def kernel(
    n_dp, n_head,
    lens_hbm, pos_hbm, q_hbm, k_hbm, v_hbm, w_hbm, qry_hbm,
    out_ref, loss_ref,
    lens, pos_ref, q_v, k_v, v_v, w_v, qall, qf, c_own, c_in, emb_slot, stat, qw_own, qw_in, uw_own, uw_in,
    a_ref, load_sem, qload_sem, q_send, q_recv, e_send, e_recv, s_send, s_recv,
    p_send, p_recv,
):
    dp = lax.axis_index("dp")
    head = lax.axis_index("head")
    side = lax.rem(head, 2)
    partner = head + 1 - 2 * side
    seq, width = q_v.shape
    heads = width // HD
    half = HD // 2
    group = HEADS // KV_HEADS
    docs = lens.shape[1]
    rows = qall.shape[1]
    nq = n_dp * rows
    kv_cols = pl.ds(pl.multiple_of((head * heads // group) * HD, HD), HD)
    blocks = seq // LANES

    k_load = pltpu.make_async_copy(k_hbm.at[:, kv_cols], k_v, load_sem.at[0])
    v_load = pltpu.make_async_copy(v_hbm.at[:, kv_cols], v_v, load_sem.at[1])
    w_load = pltpu.make_async_copy(w_hbm, w_v, load_sem.at[2])
    qry_load = pltpu.make_async_copy(qry_hbm, qall.at[dp * n_head + head], load_sem.at[3])
    q_loads = [
        pltpu.make_async_copy(
            q_hbm.at[pl.ds(b * LANES, LANES)], q_v.at[pl.ds(b * LANES, LANES)], qload_sem.at[b]
        )
        for b in range(blocks)
    ]
    lens_load = pltpu.make_async_copy(lens_hbm, lens, load_sem.at[4])
    pos_load = pltpu.make_async_copy(pos_hbm, pos_ref, load_sem.at[5])
    lens_load.start()
    k_load.start()
    q_loads[0].start()
    qry_load.start()
    for load in q_loads[1:]:
        load.start()
    v_load.start()
    w_load.start()
    pos_load.start()

    barrier = pltpu.get_barrier_semaphore()

    def peer(me, k, n):
        return lax.bitwise_xor(me, n - k)

    def everyone(body):
        for x in reversed(range(n_head)):
            each(0 if x else 1, n_dp, lambda k: body(lax.bitwise_xor(head, x), lax.bitwise_xor(dp, n_dp - 1 - k) if x else lax.bitwise_xor(dp, n_dp - k)))

    everyone(lambda h, d: pl.semaphore_signal(
        barrier, inc=1, device_id={"dp": d, "head": h}, device_id_type=pl.DeviceIdType.MESH
    ))
    peers = n_dp * n_head - 1
    mine = qall.at[dp * n_head + head]

    def q_copy(h, d):
        return pltpu.make_async_remote_copy(
            src_ref=mine, dst_ref=mine, send_sem=q_send, recv_sem=q_recv,
            device_id={"dp": d, "head": h}, device_id_type=pl.DeviceIdType.MESH,
        )

    def queries_to(h):
        @pl.when(head != h)
        def _():
            q_copy(h, dp).start()

        each(1, n_dp, lambda k: q_copy(h, peer(dp, k, n_dp)).start())

    def e_copy(h):
        slot = emb_slot.at[head]
        return remote(slot, slot, e_send, e_recv, "head", h)

    def s_copy(k, owner):
        slot = stat.at[owner]
        return remote(slot, slot, s_send, s_recv, "dp", peer(dp, k, n_dp))

    ii = lax.broadcasted_iota(jnp.int32, (1, seq), 1)
    drow = lax.broadcasted_iota(jnp.int32, (docs, 1), 0)
    start_row = jnp.zeros((1, seq), jnp.int32)
    starts = jnp.zeros((docs, 1), jnp.int32)
    lens_col = jnp.zeros((docs, 1), jnp.int32)
    begin = jnp.int32(0)
    lens_load.wait()
    for d in range(docs):
        start_row = jnp.where(ii >= begin, begin, start_row)
        starts = jnp.where(drow == d, begin, starts)
        lens_col = jnp.where(drow == d, lens[0, d], lens_col)
        begin = begin + lens[0, d]
    len_f = lens_col.astype(f32)
    member = (ii >= starts) & (ii < starts + lens_col)

    k_load.wait()
    rate = math.log2(math.e) / math.sqrt(HD)
    reach = (LONGEST + LANES - 2) // LANES
    weights = [[None] * blocks for _ in range(heads)]
    for b in range(blocks):
        q_loads[b].wait()
        cols = slice(b * LANES, (b + 1) * LANES)
        first = max(0, b - reach)
        allowed = []
        for j in range(first, b + 1):
            jj = lax.broadcasted_iota(jnp.int32, (LANES, LANES), 0) + j * LANES
            ok = jj >= start_row[:, cols]
            allowed.append(ok & (jj <= ii[:, cols]) if j == b else ok)
        allowed = jnp.concatenate(allowed, axis=0)
        for h in range(heads):
            s = mm(k_v[first * LANES:(b + 1) * LANES, :], q_v[cols, h * HD:(h + 1) * HD], NT)
            s = jnp.where(allowed, s, -1e30)
            e = jnp.exp2((s - jnp.max(s, axis=0, keepdims=True)) * rate)
            p = e * (1.0 / jnp.sum(e, axis=0, keepdims=True))
            for j in range(first, b + 1):
                piece = p[(j - first) * LANES:(j - first + 1) * LANES]
                weights[h][j] = piece if weights[h][j] is None else weights[h][j] + piece

    def keys_of(x):
        x = jnp.sum(x.T, axis=0, keepdims=True)
        return jnp.broadcast_to(x, (docs, LANES))

    csum = [jnp.concatenate([keys_of(x) for x in weights[h]], axis=1) for h in range(heads)]
    spread = jnp.concatenate([jnp.where(member, csum[h], 0.0) for h in range(heads)], axis=0)
    s_hi, s_lo = hi_lo(spread)
    qry_load.wait()
    pl.semaphore_wait(barrier, peers)
    queries_to(0)
    queries_to(1)
    v_load.wait()
    span = heads * docs
    pooled = mm(jnp.concatenate([s_hi, s_lo], axis=0), v_v[...], NN)
    pooled = pooled[:span] + pooled[span:]
    pooled = jnp.concatenate(
        [pooled[h * docs:(h + 1) * docs] for h in range(heads)], axis=1
    ) / len_f
    p_hi, p_lo = hi_lo(pooled)
    w_load.wait()
    emb = mm(jnp.concatenate([p_hi, p_lo], axis=0), w_v[...], NN)
    emb_slot[head] = (emb[:docs] + emb[docs:]).astype(bf16)
    for h in range(n_head):
        @pl.when(head != h)
        def _():
            e_copy(h).start()

    for h in range(2, n_head):
        queries_to(h)

    rid = lax.broadcasted_iota(jnp.int32, (c_own.shape[0], 1), 0)
    packed = jnp.zeros(c_own.shape, f32)
    for h in range(heads):
        packed = jnp.where(rid == h, csum[h][:c_own.shape[0]], packed)
    c_own[...] = packed
    c_copy = remote(c_own, c_in, p_send.at[0], p_recv.at[0], "head", partner)
    c_copy.start()
    wait_all(qall.at[pl.ds(0, peers)], q_recv)
    pack = max(1, SUBLANES // rows)

    def assemble(t):
        for o in range(n_head):
            piece = jnp.concatenate([qall[(t * pack + u) * n_head + o].astype(f32) for u in range(pack)], axis=0)
            qf[pl.ds(t * pack * rows, pack * rows), o * width:(o + 1) * width] = piece

    each(0, n_dp // pack, assemble)
    qmat = qf[...].astype(bf16)

    def w_half(which):
        return jnp.concatenate(
            [w_v[pl.ds(pl.multiple_of(h * HD + which * half, half), half), :] for h in range(heads)], axis=0
        )

    pos_load.wait()
    chosen = (pos_ref[...] == dp * docs + drow).astype(f32)

    wait_all(emb_slot.at[pl.ds(0, n_head - 1)], e_recv)
    emb = emb_slot[0].astype(f32)
    for o in range(1, n_head):
        emb = emb + emb_slot[o].astype(f32)
    rnorm = 1.0 / jnp.sqrt(jnp.sum(emb * emb, axis=1, keepdims=True) + 1e-06)
    unit = emb * rnorm
    u_hi, u_lo = hi_lo(unit)
    u_both = jnp.concatenate([u_hi, u_lo], axis=0)
    sims = sim_scale * mm(u_both, qmat, NT)
    logits = sims[:docs]
    full = logits + sims[docs:]
    top = jnp.max(logits, axis=0, keepdims=True)
    total = jnp.sum(jnp.exp(logits - top), axis=0, keepdims=True)
    hit = jnp.sum(logits * chosen, axis=0, keepdims=True)
    srow = lax.broadcasted_iota(jnp.int32, (stat.shape[1], 1), 0)
    stat[dp] = jnp.where(srow == 0, top, jnp.where(srow == 1, total, hit))
    each(1, n_dp, lambda k: s_copy(k, dp).start())

    lhs = jnp.concatenate([qmat, u_both], axis=0)
    proj = mm(lhs, w_half(1 - side), NT)
    qw_own[...] = proj[:nq].astype(bf16)
    qw_copy = remote(qw_own, qw_in, p_send.at[1], p_recv.at[1], "head", partner)
    qw_copy.start()
    uw_own[...] = proj[nq:nq + docs] + proj[nq + docs:]
    uw_copy = remote(uw_own, uw_in, p_send.at[2], p_recv.at[2], "head", partner)
    uw_copy.start()
    proj = mm(lhs, w_half(side), NT)
    qw_mine = proj[:nq].astype(bf16)
    uw = proj[nq:nq + docs] + proj[nq + docs:]
    factor = rnorm * (loss_scale / len_f)

    c_copy.wait_recv()
    other = jnp.concatenate(
        [jnp.where(member, c_in[h:h + 1, :], 0.0) for h in range(heads)], axis=0
    )
    both = jnp.concatenate([spread, other], axis=0)
    b_hi, b_lo = hi_lo(both)
    a_ref[...] = jnp.concatenate([b_hi, b_lo], axis=0)

    wait_all(stat.at[pl.ds(0, n_dp - 1)], s_recv)
    top = fold(
        n_dp, lambda k, c: jnp.maximum(c, stat[k][0:1]), jnp.full((1, nq), -jnp.inf, f32)
    )

    def gather(k, c):
        tile = stat[k]
        return c[0] + tile[1:2] * jnp.exp(tile[0:1] - top), c[1] + tile[2:3]

    zero = jnp.zeros((1, nq), f32)
    total, hit = fold(n_dp, gather, (zero, zero))
    lse = top + jnp.log(total)
    loss_ref[0, 0] = jnp.sum(lse - hit) * (1.0 / nq)
    dl = jnp.exp(logits - lse) - chosen
    inner = jnp.sum(dl * full, axis=1, keepdims=True)
    d_hi, d_lo = hi_lo(dl)
    qw_copy.wait_recv()
    qw = jnp.concatenate([qw_mine, qw_in[...]], axis=1)
    qw2 = jnp.concatenate([qw, qw], axis=0)
    g = sim_scale * mm(jnp.concatenate([d_hi, d_lo], axis=1), qw2, NN)
    uw_copy.wait_recv()
    uw2 = jnp.concatenate([uw, uw_in[...]], axis=1)
    g = factor * (g - inner * uw2)
    small = jnp.concatenate(
        [g[:, h * half:(h + 1) * half] for h in range(2 * heads)], axis=0
    )
    small = jnp.concatenate([small, small], axis=0).T.astype(bf16)
    out_ref[...] = mm(small, a_ref[...], NN).astype(bf16)

    wait_all(qall.at[pl.ds(0, peers)], q_send)
    wait_all(emb_slot.at[pl.ds(0, n_head - 1)], e_send)
    wait_all(stat.at[pl.ds(0, n_dp - 1)], s_send)
    c_copy.wait_send()
    qw_copy.wait_send()
    uw_copy.wait_send()


def store(x_ref, l_ref, o_ref, lo_ref, sem):
    copies = [
        pltpu.make_async_copy(x_ref, o_ref, sem.at[0]),
        pltpu.make_async_copy(l_ref, lo_ref, sem.at[1]),
    ]
    for copy in copies:
        copy.start()
    for copy in copies:
        copy.wait()


def per_device(n_dp, n_head, attn_queries, keys, values, out_weight, lengths, queries, positives):
    seq, width = attn_queries.shape
    heads = width // HD
    docs = lengths.shape[1]
    rows = queries.shape[0]
    nq = n_dp * rows
    model = out_weight.shape[1]
    blocks = seq // LANES
    half = width // 2
    dma = pltpu.SemaphoreType.DMA
    hbm = pl.BlockSpec(memory_space=pltpu.HBM)
    vmem = pl.BlockSpec(memory_space=pltpu.VMEM)
    smem = pl.BlockSpec(memory_space=pltpu.SMEM)
    d_values, loss = pl.pallas_call(
        functools.partial(kernel, n_dp, n_head),
        out_shape=(
            pltpu.VMEM((HD // 2, seq), bf16),
            pltpu.SMEM((1, 1), f32),
        ),
        in_specs=[hbm, hbm, hbm, hbm, hbm, hbm, hbm],
        out_specs=(vmem, smem),
        scratch_shapes=[
            pltpu.SMEM((1, docs), jnp.int32),
            pltpu.VMEM((1, nq), jnp.int32),
            pltpu.VMEM((seq, width), bf16),
            pltpu.VMEM((seq, HD), bf16),
            pltpu.VMEM((seq, HD), bf16),
            pltpu.VMEM((width, model), bf16),
            pltpu.VMEM((n_dp * n_head, rows, width), bf16),
            pltpu.VMEM((nq, model), f32),
            pltpu.VMEM((SUBLANES // 2, seq), f32),
            pltpu.VMEM((SUBLANES // 2, seq), f32),
            pltpu.VMEM((n_head, docs, model), bf16),
            pltpu.VMEM((n_dp, SUBLANES // 2, nq), f32),
            pltpu.VMEM((nq, half), bf16),
            pltpu.VMEM((nq, half), bf16),
            pltpu.VMEM((docs, half), f32),
            pltpu.VMEM((docs, half), f32),
            pltpu.VMEM((4 * heads * docs, seq), bf16),
            dma((6,)),
            dma((blocks,)),
            dma,
            dma,
            dma,
            dma,
            dma,
            dma,
            dma((3,)),
            dma((3,)),
        ],
        compiler_params=pltpu.CompilerParams(collective_id=0, has_side_effects=True),
    )(lengths, positives.reshape(1, nq), attn_queries, keys, values, out_weight, queries)
    d_values = pltpu.with_memory_space_constraint(d_values, pltpu.VMEM)
    loss = pltpu.with_memory_space_constraint(loss, pltpu.SMEM)
    d_values, loss = pl.pallas_call(
        store,
        out_shape=(
            jax.ShapeDtypeStruct((HD // 2, seq), bf16),
            jax.ShapeDtypeStruct((1, 1), f32),
        ),
        in_specs=[vmem, smem],
        out_specs=(hbm, hbm),
        scratch_shapes=[dma((2,))],
    )(d_values, loss)
    return d_values.T, loss.reshape(())


def solution(mesh):
    placed = (
        P("dp", "head"),
        P("dp", None),
        P("dp", None),
        P("head", None),
        P("dp", None),
        P("dp", "head"),
        P(),
    )
    return jax.shard_map(
        functools.partial(per_device, mesh.shape["dp"], mesh.shape["head"]),
        mesh=mesh, in_specs=placed, out_specs=(P("dp", "head"), P()), check_vma=False,
    )
```

```python
import functools
import math

import jax
import jax.numpy as jnp
from jax import lax
from jax.experimental import pallas as pl
from jax.experimental.pallas import tpu as pltpu
from jax.sharding import PartitionSpec as P

HEADS = 12
KV_HEADS = 2
HD = 128
LANES = 128
SUBLANES = 8
LONGEST = 256

sim_scale = 20.0
loss_scale = 32768.0

NT = (((1,), (1,)), ((), ()))
NN = (((1,), (0,)), ((), ()))
f32 = jnp.float32
bf16 = jnp.bfloat16


def mm(a, b, dims):
    return lax.dot_general(a, b, dims, preferred_element_type=f32)


def hi_lo(x):
    hi = x.astype(bf16)
    return hi, (x - hi.astype(f32)).astype(bf16)


def each(first, last, body):
    if last - first <= 8:
        for k in range(first, last):
            body(k)
    else:
        lax.fori_loop(first, last, lambda k, c: (body(k), c)[1], 0)


def fold(last, body, carry):
    if last <= 8:
        for k in range(last):
            carry = body(k, carry)
        return carry
    return lax.fori_loop(0, last, body, carry)


def remote(src, dst, send, recv, axis, peer):
    return pltpu.make_async_remote_copy(
        src_ref=src, dst_ref=dst, send_sem=send, recv_sem=recv,
        device_id={axis: peer}, device_id_type=pl.DeviceIdType.MESH,
    )


def wait_all(ref, sem):
    pltpu.make_async_copy(ref, ref, sem).wait()


def kernel(
    n_dp, n_head,
    lens_hbm, pos_hbm, q_hbm, k_hbm, v_hbm, w_hbm, qry_hbm,
    out_ref, loss_ref,
    lens, pos_ref, q_v, k_v, v_v, w_v, qall, qf, c_own, c_in, emb_slot, stat, qw_own, qw_in, uw_own, uw_in,
    a_ref, e_sum, hello, load_sem, qload_sem, q_send, q_recv, e_send, e_recv, s_send, s_recv,
    p_send, p_recv,
):
    dp = lax.axis_index("dp")
    head = lax.axis_index("head")
    side = lax.rem(head, 2)
    partner = head + 1 - 2 * side
    seq, width = q_v.shape
    heads = width // HD
    half = HD // 2
    group = HEADS // KV_HEADS
    docs = lens.shape[1]
    rows = qall.shape[1]
    nq = n_dp * rows
    kv_cols = pl.ds(pl.multiple_of((head * heads // group) * HD, HD), HD)
    blocks = seq // LANES

    k_load = pltpu.make_async_copy(k_hbm.at[:, kv_cols], k_v, load_sem.at[0])
    v_load = pltpu.make_async_copy(v_hbm.at[:, kv_cols], v_v, load_sem.at[1])
    w_load = pltpu.make_async_copy(w_hbm, w_v, load_sem.at[2])
    qry_load = pltpu.make_async_copy(qry_hbm, qall.at[dp * n_head + head], load_sem.at[3])
    q_load = pltpu.make_async_copy(q_hbm, q_v, qload_sem)
    lens_load = pltpu.make_async_copy(lens_hbm, lens, load_sem.at[4])
    pos_load = pltpu.make_async_copy(pos_hbm, pos_ref, load_sem.at[5])
    lens_load.start()
    k_load.start()
    qry_load.start()
    q_load.start()
    v_load.start()
    w_load.start()
    pos_load.start()

    barrier = pltpu.get_barrier_semaphore()

    def peer(me, k, n):
        return lax.bitwise_xor(me, n - k)

    rank = head * n_dp + dp

    def ranks(first, last, body):
        lax.fori_loop(first, last, lambda f, c: (body(lax.div(f, n_dp), lax.rem(f, n_dp)), c)[1], 0)

    def signal(semaphore, h, d):
        pl.semaphore_signal(
            semaphore, inc=1, device_id={"dp": d, "head": h}, device_id_type=pl.DeviceIdType.MESH
        )

    ranks(rank + 1, n_dp * n_head, lambda h, d: signal(barrier, h, d))
    peers = n_dp * n_head - 1
    mine = qall.at[dp * n_head + head]

    def q_copy(h, d):
        return pltpu.make_async_remote_copy(
            src_ref=mine, dst_ref=mine, send_sem=q_send, recv_sem=q_recv,
            device_id={"dp": d, "head": h}, device_id_type=pl.DeviceIdType.MESH,
        )

    def e_copy(h):
        slot = emb_slot.at[head]
        return remote(slot, slot, e_send, e_recv.at[head], "head", h)

    def e_from(h):
        return remote(emb_slot.at[h], emb_slot.at[h], e_send, e_recv.at[h], "head", h)

    def sum_copy(h):
        return remote(e_sum, emb_slot.at[1], e_send, e_recv.at[1], "head", h)

    def s_copy(k, owner):
        slot = stat.at[owner]
        return remote(slot, slot, s_send, s_recv, "dp", peer(dp, k, n_dp))

    def queries(first, last):
        ranks(first, last, lambda h, d: q_copy(h, d).start())

    far = dp >= n_dp // 4

    def meet():
        @pl.when(rank > 0)
        def _():
            pl.semaphore_wait(barrier, rank)

        ranks(0, rank, lambda h, d: signal(hello.at[head], h, d))
        qry_load.wait()

    @pl.when(far)
    def _():
        meet()
        ranks(0, jnp.minimum(rank, 2 * n_dp), lambda h, d: q_copy(h, d).start())

    ii = lax.broadcasted_iota(jnp.int32, (1, seq), 1)
    drow = lax.broadcasted_iota(jnp.int32, (docs, 1), 0)
    start_row = jnp.zeros((1, seq), jnp.int32)
    starts = jnp.zeros((docs, 1), jnp.int32)
    lens_col = jnp.zeros((docs, 1), jnp.int32)
    begin = jnp.int32(0)
    lens_load.wait()
    for d in range(docs):
        start_row = jnp.where(ii >= begin, begin, start_row)
        starts = jnp.where(drow == d, begin, starts)
        lens_col = jnp.where(drow == d, lens[0, d], lens_col)
        begin = begin + lens[0, d]
    len_f = lens_col.astype(f32)
    member = (ii >= starts) & (ii < starts + lens_col)

    k_load.wait()
    rate = math.log2(math.e) / math.sqrt(HD)
    reach = (LONGEST + LANES - 2) // LANES
    weights = [[None] * blocks for _ in range(heads)]
    q_load.wait()
    for b in range(blocks):
        cols = slice(b * LANES, (b + 1) * LANES)
        first = max(0, b - reach)
        allowed = []
        for j in range(first, b + 1):
            jj = lax.broadcasted_iota(jnp.int32, (LANES, LANES), 0) + j * LANES
            ok = jj >= start_row[:, cols]
            allowed.append(ok & (jj <= ii[:, cols]) if j == b else ok)
        allowed = jnp.concatenate(allowed, axis=0)
        for h in range(heads):
            s = mm(k_v[first * LANES:(b + 1) * LANES, :], q_v[cols, h * HD:(h + 1) * HD], NT)
            s = jnp.where(allowed, s, -1e30)
            e = jnp.exp2((s - jnp.max(s, axis=0, keepdims=True)) * rate)
            p = e * (1.0 / jnp.sum(e, axis=0, keepdims=True))
            for j in range(first, b + 1):
                piece = p[(j - first) * LANES:(j - first + 1) * LANES]
                weights[h][j] = piece if weights[h][j] is None else weights[h][j] + piece

    def keys_of(x):
        x = jnp.sum(x.T, axis=0, keepdims=True)
        return jnp.broadcast_to(x, (docs, LANES))

    csum = [jnp.concatenate([keys_of(x) for x in weights[h]], axis=1) for h in range(heads)]
    spread = jnp.concatenate([jnp.where(member, csum[h], 0.0) for h in range(heads)], axis=0)
    s_hi, s_lo = hi_lo(spread)
    v_load.wait()
    span = heads * docs
    pooled = mm(jnp.concatenate([s_hi, s_lo], axis=0), v_v[...], NN)
    pooled = pooled[:span] + pooled[span:]
    pooled = jnp.concatenate(
        [pooled[h * docs:(h + 1) * docs] for h in range(heads)], axis=1
    ) / len_f
    p_hi, p_lo = hi_lo(pooled)
    w_load.wait()
    emb = mm(jnp.concatenate([p_hi, p_lo], axis=0), w_v[...], NN)
    emb_slot[head] = (emb[:docs] + emb[docs:]).astype(bf16)
    pl.when(jnp.logical_not(far))(meet)
    ahead = jnp.logical_and(head >= 2, jnp.logical_not(far))

    @pl.when(ahead)
    def _():
        queries(0, n_dp)
        e_copy(1).start()
        queries(n_dp, 2 * n_dp)
        e_copy(0).start()

    def plane(t, carry):
        base = t * n_dp
        inside = t == head

        @pl.when(t > head)
        def _():
            pl.semaphore_wait(hello.at[t], n_dp)

        @pl.when(jnp.logical_and(t != head, jnp.logical_or(t < head, jnp.logical_or(head >= 2, t + head == 1))))
        def _():
            e_copy(t).start()

        last = jnp.where(inside, dp, n_dp)
        sent = jnp.logical_and(far, jnp.logical_and(t < 2, t <= head))
        ranks(base, base + jnp.where(sent, 0, last), lambda h, d: q_copy(h, d).start())

        @pl.when(jnp.logical_and(inside, dp < n_dp - 1))
        def _():
            pl.semaphore_wait(hello.at[t], n_dp - 1 - dp)
            ranks(base + dp + 1, base + n_dp, lambda h, d: q_copy(h, d).start())

        return carry

    lax.fori_loop(jnp.where(ahead, 2, 0), n_head, plane, 0)

    @pl.when(head == 1)
    def _():
        e_from(0).wait_recv()
        e_sum[...] = (emb_slot[0].astype(f32) + emb_slot[1].astype(f32)).astype(bf16)
        each(2, n_head, lambda h: sum_copy(h).start())

    @pl.when(head >= 2)
    def _():
        emb_slot[0] = jnp.zeros(emb_slot.shape[1:], bf16)

    rid = lax.broadcasted_iota(jnp.int32, (c_own.shape[0], 1), 0)
    packed = jnp.zeros(c_own.shape, f32)
    for h in range(heads):
        packed = jnp.where(rid == h, csum[h][:c_own.shape[0]], packed)
    c_own[...] = packed
    c_copy = remote(c_own, c_in, p_send.at[0], p_recv.at[0], "head", partner)
    c_copy.start()
    wait_all(qall.at[pl.ds(0, peers)], q_recv)
    pack = max(1, SUBLANES // rows)

    def assemble(t):
        for o in range(n_head):
            piece = jnp.concatenate([qall[(t * pack + u) * n_head + o].astype(f32) for u in range(pack)], axis=0)
            qf[pl.ds(t * pack * rows, pack * rows), o * width:(o + 1) * width] = piece

    each(0, n_dp // pack, assemble)
    qmat = qf[...].astype(bf16)

    def w_half(which):
        return jnp.concatenate(
            [w_v[pl.ds(pl.multiple_of(h * HD + which * half, half), half), :] for h in range(heads)], axis=0
        )

    pos_load.wait()
    chosen = (pos_ref[...] == dp * docs + drow).astype(f32)

    pl.when(head == 0)(lambda: e_from(1).wait_recv())
    pl.when(head >= 2)(lambda: e_from(1).wait_recv())
    for h in range(2, n_head):
        pl.when(head != h)(lambda: e_from(h).wait_recv())
    emb = emb_slot[0].astype(f32)
    for o in range(1, n_head):
        emb = emb + emb_slot[o].astype(f32)
    rnorm = 1.0 / jnp.sqrt(jnp.sum(emb * emb, axis=1, keepdims=True) + 1e-06)
    unit = emb * rnorm
    u_hi, u_lo = hi_lo(unit)
    u_both = jnp.concatenate([u_hi, u_lo], axis=0)
    lhs = jnp.concatenate([qmat, u_both], axis=0)
    qw_copy = remote(qw_own, qw_in, p_send.at[1], p_recv.at[1], "head", partner)
    uw_copy = remote(uw_own, uw_in, p_send.at[2], p_recv.at[2], "head", partner)

    def project():
        proj = mm(lhs, w_half(1 - side), NT)
        qw_own[...] = proj[:nq].astype(bf16)
        qw_copy.start()
        uw_own[...] = proj[nq:nq + docs] + proj[nq + docs:]
        uw_copy.start()

    pl.when(side == 1)(project)
    sims = sim_scale * mm(u_both, qmat, NT)
    logits = sims[:docs]
    full = logits + sims[docs:]
    top = jnp.max(logits, axis=0, keepdims=True)
    total = jnp.sum(jnp.exp(logits - top), axis=0, keepdims=True)
    hit = jnp.sum(logits * chosen, axis=0, keepdims=True)
    srow = lax.broadcasted_iota(jnp.int32, (stat.shape[1], 1), 0)
    stat[dp] = jnp.where(srow == 0, top, jnp.where(srow == 1, total, hit))
    each(1, n_dp, lambda k: s_copy(k, dp).start())

    pl.when(side == 0)(project)
    proj = mm(lhs, w_half(side), NT)
    qw_mine = proj[:nq].astype(bf16)
    uw = proj[nq:nq + docs] + proj[nq + docs:]
    factor = rnorm * (loss_scale / len_f)

    c_copy.wait_recv()
    other = jnp.concatenate(
        [jnp.where(member, c_in[h:h + 1, :], 0.0) for h in range(heads)], axis=0
    )
    both = jnp.concatenate([spread, other], axis=0)
    b_hi, b_lo = hi_lo(both)
    a_ref[...] = jnp.concatenate([b_hi, b_lo], axis=0)

    qw_copy.wait_recv()
    qw = jnp.concatenate([qw_mine, qw_in[...]], axis=1)
    qw2 = jnp.concatenate([qw, qw], axis=0)
    uw_copy.wait_recv()
    uw2 = factor * jnp.concatenate([uw, uw_in[...]], axis=1)
    factor = factor * sim_scale

    wait_all(stat.at[pl.ds(0, n_dp - 1)], s_recv)
    top = fold(
        n_dp, lambda k, c: jnp.maximum(c, stat[k][0:1]), jnp.full((1, nq), -jnp.inf, f32)
    )
    shifted = jnp.exp(logits - top)

    def gather(k, c):
        tile = stat[k]
        return c[0] + tile[1:2] * jnp.exp(tile[0:1] - top), c[1] + tile[2:3]

    zero = jnp.zeros((1, nq), f32)
    total, hit = fold(n_dp, gather, (zero, zero))
    dl = shifted * (1.0 / total) - chosen
    d_hi, d_lo = hi_lo(dl)
    g = mm(jnp.concatenate([d_hi, d_lo], axis=1), qw2, NN)
    inner = jnp.sum(dl * full, axis=1, keepdims=True)
    loss_ref[0, 0] = jnp.sum(top + jnp.log(total) - hit) * (1.0 / nq)
    g = factor * g - inner * uw2
    small = jnp.concatenate(
        [g[:, h * half:(h + 1) * half] for h in range(2 * heads)], axis=0
    )
    small = jnp.concatenate([small, small], axis=0).T.astype(bf16)
    out_ref[...] = mm(small, a_ref[...], NN).astype(bf16)

    wait_all(qall.at[pl.ds(0, peers)], q_send)
    pl.when(head == 0)(lambda: wait_all(emb_slot.at[0], e_send))
    pl.when(head > 0)(lambda: wait_all(emb_slot.at[pl.ds(0, n_head - 1)], e_send))
    wait_all(stat.at[pl.ds(0, n_dp - 1)], s_send)
    c_copy.wait_send()
    qw_copy.wait_send()
    uw_copy.wait_send()


def store(x_ref, l_ref, o_ref, lo_ref, sem):
    copies = [
        pltpu.make_async_copy(x_ref, o_ref, sem.at[0]),
        pltpu.make_async_copy(l_ref, lo_ref, sem.at[1]),
    ]
    for copy in copies:
        copy.start()
    for copy in copies:
        copy.wait()


def per_device(n_dp, n_head, attn_queries, keys, values, out_weight, lengths, queries, positives):
    seq, width = attn_queries.shape
    heads = width // HD
    docs = lengths.shape[1]
    rows = queries.shape[0]
    nq = n_dp * rows
    model = out_weight.shape[1]
    blocks = seq // LANES
    half = width // 2
    dma = pltpu.SemaphoreType.DMA
    hbm = pl.BlockSpec(memory_space=pltpu.HBM)
    vmem = pl.BlockSpec(memory_space=pltpu.VMEM)
    smem = pl.BlockSpec(memory_space=pltpu.SMEM)
    d_values, loss = pl.pallas_call(
        functools.partial(kernel, n_dp, n_head),
        out_shape=(
            pltpu.VMEM((HD // 2, seq), bf16),
            pltpu.SMEM((1, 1), f32),
        ),
        in_specs=[hbm, hbm, hbm, hbm, hbm, hbm, hbm],
        out_specs=(vmem, smem),
        scratch_shapes=[
            pltpu.SMEM((1, docs), jnp.int32),
            pltpu.VMEM((1, nq), jnp.int32),
            pltpu.VMEM((seq, width), bf16),
            pltpu.VMEM((seq, HD), bf16),
            pltpu.VMEM((seq, HD), bf16),
            pltpu.VMEM((width, model), bf16),
            pltpu.VMEM((n_dp * n_head, rows, width), bf16),
            pltpu.VMEM((nq, model), f32),
            pltpu.VMEM((SUBLANES // 2, seq), f32),
            pltpu.VMEM((SUBLANES // 2, seq), f32),
            pltpu.VMEM((n_head, docs, model), bf16),
            pltpu.VMEM((n_dp, SUBLANES // 2, nq), f32),
            pltpu.VMEM((nq, half), bf16),
            pltpu.VMEM((nq, half), bf16),
            pltpu.VMEM((docs, half), f32),
            pltpu.VMEM((docs, half), f32),
            pltpu.VMEM((4 * heads * docs, seq), bf16),
            pltpu.VMEM((docs, model), bf16),
            pltpu.SemaphoreType.REGULAR((n_head,)),
            dma((6,)),
            dma,
            dma,
            dma,
            dma,
            dma((n_head,)),
            dma,
            dma,
            dma((3,)),
            dma((3,)),
        ],
        compiler_params=pltpu.CompilerParams(collective_id=0, has_side_effects=True),
    )(lengths, positives.reshape(1, nq), attn_queries, keys, values, out_weight, queries)
    d_values = pltpu.with_memory_space_constraint(d_values, pltpu.VMEM)
    loss = pltpu.with_memory_space_constraint(loss, pltpu.SMEM)
    d_values, loss = pl.pallas_call(
        store,
        out_shape=(
            jax.ShapeDtypeStruct((HD // 2, seq), bf16),
            jax.ShapeDtypeStruct((1, 1), f32),
        ),
        in_specs=[vmem, smem],
        out_specs=(hbm, hbm),
        scratch_shapes=[dma((2,))],
    )(d_values, loss)
    return d_values.T, loss.reshape(())


def solution(mesh):
    placed = (
        P("dp", "head"),
        P("dp", None),
        P("dp", None),
        P("head", None),
        P("dp", None),
        P("dp", "head"),
        P(),
    )
    return jax.shard_map(
        functools.partial(per_device, mesh.shape["dp"], mesh.shape["head"]),
        mesh=mesh, in_specs=placed, out_specs=(P("dp", "head"), P()), check_vma=False,
    )
```

```python
import functools
import math

import jax
import jax.numpy as jnp
from jax import lax
from jax.experimental import pallas as pl
from jax.experimental.pallas import tpu as pltpu
from jax.sharding import PartitionSpec as P

HEADS = 12
KV_HEADS = 2
HD = 128
LANES = 128
SUBLANES = 8
LONGEST = 256

sim_scale = 20.0
loss_scale = 32768.0

NT = (((1,), (1,)), ((), ()))
NN = (((1,), (0,)), ((), ()))
f32 = jnp.float32
bf16 = jnp.bfloat16


def mm(a, b, dims):
    return lax.dot_general(a, b, dims, preferred_element_type=f32)


def hi_lo(x):
    hi = x.astype(bf16)
    return hi, (x - hi.astype(f32)).astype(bf16)


def each(first, last, body):
    if last - first <= 8:
        for k in range(first, last):
            body(k)
    else:
        lax.fori_loop(first, last, lambda k, c: (body(k), c)[1], 0)


def fold(last, body, carry):
    if last <= 8:
        for k in range(last):
            carry = body(k, carry)
        return carry
    return lax.fori_loop(0, last, body, carry)


def remote(src, dst, send, recv, axis, peer):
    return pltpu.make_async_remote_copy(
        src_ref=src, dst_ref=dst, send_sem=send, recv_sem=recv,
        device_id={axis: peer}, device_id_type=pl.DeviceIdType.MESH,
    )


def wait_all(ref, sem):
    pltpu.make_async_copy(ref, ref, sem).wait()


def kernel(
    n_dp, n_head,
    lens_hbm, pos_hbm, q_hbm, k_hbm, v_hbm, w_hbm, qry_hbm,
    out_ref, loss_ref,
    lens, pos_ref, q_v, k_v, v_v, w_v, qall, qf, c_own, c_in, emb_slot, stat, qw_own, qw_in, uw_own, uw_in,
    a_ref, e_sum, hello, load_sem, qload_sem, send, q_recv, e_recv, s_recv,
    p_recv,
):
    dp = lax.axis_index("dp")
    head = lax.axis_index("head")
    side = lax.rem(head, 2)
    partner = head + 1 - 2 * side
    seq, width = q_v.shape
    heads = width // HD
    half = HD // 2
    group = HEADS // KV_HEADS
    docs = lens.shape[1]
    rows = qall.shape[1]
    nq = n_dp * rows
    kv_cols = pl.ds(pl.multiple_of((head * heads // group) * HD, HD), HD)
    blocks = seq // LANES

    k_load = pltpu.make_async_copy(k_hbm.at[:, kv_cols], k_v, load_sem.at[0])
    v_load = pltpu.make_async_copy(v_hbm.at[:, kv_cols], v_v, load_sem.at[1])
    w_load = pltpu.make_async_copy(w_hbm, w_v, load_sem.at[2])
    qry_load = pltpu.make_async_copy(qry_hbm, qall.at[dp * n_head + head], load_sem.at[3])
    q_load = pltpu.make_async_copy(q_hbm, q_v, qload_sem)
    lens_load = pltpu.make_async_copy(lens_hbm, lens, load_sem.at[4])
    pos_load = pltpu.make_async_copy(pos_hbm, pos_ref, load_sem.at[1])
    lens_load.start()
    k_load.start()
    qry_load.start()
    q_load.start()
    v_load.start()
    w_load.start()
    pos_load.start()

    barrier = pltpu.get_barrier_semaphore()

    def peer(me, k, n):
        return lax.bitwise_xor(me, n - k)

    rank = head * n_dp + dp

    def ranks(first, last, body):
        lax.fori_loop(first, last, lambda f, c: (body(lax.div(f, n_dp), lax.rem(f, n_dp)), c)[1], 0)

    def signal(semaphore, h, d):
        pl.semaphore_signal(
            semaphore, inc=1, device_id={"dp": d, "head": h}, device_id_type=pl.DeviceIdType.MESH
        )

    ranks(rank + 1, n_dp * n_head, lambda h, d: signal(barrier, h, d))
    peers = n_dp * n_head - 1
    mine = qall.at[dp * n_head + head]

    def q_copy(h, d):
        return pltpu.make_async_remote_copy(
            src_ref=mine, dst_ref=mine, send_sem=send, recv_sem=q_recv,
            device_id={"dp": d, "head": h}, device_id_type=pl.DeviceIdType.MESH,
        )

    def e_copy(h):
        slot = emb_slot.at[head]
        return remote(slot, slot, send, e_recv.at[jnp.minimum(head, 1)], "head", h)

    def e_from(h):
        return remote(emb_slot.at[h], emb_slot.at[h], send, e_recv.at[min(h, 1)], "head", h)

    def sum_copy(h):
        return remote(e_sum, emb_slot.at[1], send, e_recv.at[1], "head", h)

    def s_copy(k, owner):
        slot = stat.at[owner]
        return remote(slot, slot, send, s_recv, "dp", peer(dp, k, n_dp))

    def queries(first, last):
        ranks(first, last, lambda h, d: q_copy(h, d).start())

    far = dp >= n_dp // 4

    def meet():
        @pl.when(rank > 0)
        def _():
            pl.semaphore_wait(barrier, rank)

    def greet():
        ranks(0, rank, lambda h, d: signal(hello.at[head], h, d))

    @pl.when(far)
    def _():
        meet()
        greet()
        qry_load.wait()
        ranks(0, jnp.minimum(rank, 2 * n_dp), lambda h, d: q_copy(h, d).start())

    ii = lax.broadcasted_iota(jnp.int32, (1, seq), 1)
    drow = lax.broadcasted_iota(jnp.int32, (docs, 1), 0)
    start_row = jnp.zeros((1, seq), jnp.int32)
    starts = jnp.zeros((docs, 1), jnp.int32)
    lens_col = jnp.zeros((docs, 1), jnp.int32)
    begin = jnp.int32(0)
    lens_load.wait()
    for d in range(docs):
        start_row = jnp.where(ii >= begin, begin, start_row)
        starts = jnp.where(drow == d, begin, starts)
        lens_col = jnp.where(drow == d, lens[0, d], lens_col)
        begin = begin + lens[0, d]
    len_f = lens_col.astype(f32)
    member = (ii >= starts) & (ii < starts + lens_col)

    k_load.wait()
    rate = math.log2(math.e) / math.sqrt(HD)
    reach = (LONGEST + LANES - 2) // LANES
    weights = [[None] * blocks for _ in range(heads)]
    q_load.wait()
    for b in range(blocks):
        cols = slice(b * LANES, (b + 1) * LANES)
        first = max(0, b - reach)
        allowed = []
        for j in range(first, b + 1):
            jj = lax.broadcasted_iota(jnp.int32, (LANES, LANES), 0) + j * LANES
            ok = jj >= start_row[:, cols]
            allowed.append(ok & (jj <= ii[:, cols]) if j == b else ok)
        allowed = jnp.concatenate(allowed, axis=0)
        for h in range(heads):
            s = mm(k_v[first * LANES:(b + 1) * LANES, :], q_v[cols, h * HD:(h + 1) * HD], NT)
            s = jnp.where(allowed, s, -1e30)
            e = jnp.exp2((s - jnp.max(s, axis=0, keepdims=True)) * rate)
            p = e * (1.0 / jnp.sum(e, axis=0, keepdims=True))
            for j in range(first, b + 1):
                piece = p[(j - first) * LANES:(j - first + 1) * LANES]
                weights[h][j] = piece if weights[h][j] is None else weights[h][j] + piece

    def keys_of(x):
        x = jnp.sum(x.T, axis=0, keepdims=True)
        return jnp.broadcast_to(x, (docs, LANES))

    csum = [jnp.concatenate([keys_of(x) for x in weights[h]], axis=1) for h in range(heads)]
    spread = jnp.concatenate([jnp.where(member, csum[h], 0.0) for h in range(heads)], axis=0)
    s_hi, s_lo = hi_lo(spread)
    v_load.wait()
    pos_load.wait()
    span = heads * docs
    pooled = mm(jnp.concatenate([s_hi, s_lo], axis=0), v_v[...], NN)
    pooled = pooled[:span] + pooled[span:]
    pooled = jnp.concatenate(
        [pooled[h * docs:(h + 1) * docs] for h in range(heads)], axis=1
    ) / len_f
    p_hi, p_lo = hi_lo(pooled)
    w_load.wait()
    emb = mm(jnp.concatenate([p_hi, p_lo], axis=0), w_v[...], NN)
    emb_slot[head] = (emb[:docs] + emb[docs:]).astype(bf16)
    @pl.when(jnp.logical_not(far))
    def _():
        meet()
        qry_load.wait()

    ahead = jnp.logical_and(head >= 2, jnp.logical_not(far))

    @pl.when(ahead)
    def _():
        queries(0, n_dp)
        e_copy(1).start()
        greet()
        queries(n_dp, 2 * n_dp)
        e_copy(0).start()

    pl.when(jnp.logical_and(head < 2, jnp.logical_not(far)))(greet)

    def plane(t, carry):
        base = t * n_dp
        inside = t == head

        @pl.when(t > head)
        def _():
            pl.semaphore_wait(hello.at[t], n_dp)

        @pl.when(jnp.logical_and(t != head, jnp.logical_or(t < head, jnp.logical_or(head >= 2, t + head == 1))))
        def _():
            e_copy(t).start()

        last = jnp.where(inside, dp, n_dp)
        sent = jnp.logical_and(far, jnp.logical_and(t < 2, t <= head))
        ranks(base, base + jnp.where(sent, 0, last), lambda h, d: q_copy(h, d).start())

        @pl.when(jnp.logical_and(inside, dp < n_dp - 1))
        def _():
            pl.semaphore_wait(hello.at[t], n_dp - 1 - dp)
            ranks(base + dp + 1, base + n_dp, lambda h, d: q_copy(h, d).start())

        return carry

    lax.fori_loop(jnp.where(ahead, 2, 0), n_head, plane, 0)

    @pl.when(head == 1)
    def _():
        e_from(0).wait_recv()
        e_sum[...] = (emb_slot[0].astype(f32) + emb_slot[1].astype(f32)).astype(bf16)
        each(2, n_head, lambda h: sum_copy(h).start())

    @pl.when(head >= 2)
    def _():
        emb_slot[0] = jnp.zeros(emb_slot.shape[1:], bf16)

    rid = lax.broadcasted_iota(jnp.int32, (c_own.shape[0], 1), 0)
    packed = jnp.zeros(c_own.shape, f32)
    for h in range(heads):
        packed = jnp.where(rid == h, csum[h][:c_own.shape[0]], packed)
    c_own[...] = packed
    c_copy = remote(c_own, c_in, send, p_recv.at[0], "head", partner)
    c_copy.start()
    wait_all(qall.at[pl.ds(0, peers)], q_recv)
    pack = max(1, SUBLANES // rows)

    def assemble(t):
        for o in range(n_head):
            piece = jnp.concatenate([qall[(t * pack + u) * n_head + o].astype(f32) for u in range(pack)], axis=0)
            qf[pl.ds(t * pack * rows, pack * rows), o * width:(o + 1) * width] = piece

    each(0, n_dp // pack, assemble)
    qmat = qf[...].astype(bf16)

    def w_half(which):
        return jnp.concatenate(
            [w_v[pl.ds(pl.multiple_of(h * HD + which * half, half), half), :] for h in range(heads)], axis=0
        )

    chosen = (pos_ref[...] == dp * docs + drow).astype(f32)

    pl.when(head == 0)(lambda: wait_all(emb_slot.at[pl.ds(0, n_head - 1)], e_recv.at[1]))
    pl.when(head > 0)(lambda: wait_all(emb_slot.at[pl.ds(0, n_head - 2)], e_recv.at[1]))
    emb = emb_slot[0].astype(f32)
    for o in range(1, n_head):
        emb = emb + emb_slot[o].astype(f32)
    rnorm = 1.0 / jnp.sqrt(jnp.sum(emb * emb, axis=1, keepdims=True) + 1e-06)
    e_both = jnp.concatenate(hi_lo(emb), axis=0)
    lhs = jnp.concatenate([qmat, e_both], axis=0)
    qw_copy = remote(qw_own, qw_in, send, p_recv.at[1], "head", partner)
    uw_copy = remote(uw_own, uw_in, send, p_recv.at[2], "head", partner)

    def project():
        proj = mm(lhs, w_half(1 - side), NT)
        qw_own[...] = proj[:nq].astype(bf16)
        qw_copy.start()
        uw_own[...] = rnorm * (proj[nq:nq + docs] + proj[nq + docs:])
        uw_copy.start()

    pl.when(side == 1)(project)
    sims = mm(e_both, qmat, NT)
    logits = (sim_scale * rnorm) * (sims[:docs] + sims[docs:])
    top = jnp.max(logits, axis=0, keepdims=True)
    total = jnp.sum(jnp.exp(logits - top), axis=0, keepdims=True)
    hit = jnp.sum(logits * chosen, axis=0, keepdims=True)
    srow = lax.broadcasted_iota(jnp.int32, (stat.shape[1], 1), 0)
    stat[dp] = jnp.where(srow == 0, top, jnp.where(srow == 1, total, hit))
    each(1, n_dp, lambda k: s_copy(k, dp).start())

    pl.when(side == 0)(project)
    proj = mm(lhs, w_half(side), NT)
    qw_mine = proj[:nq].astype(bf16)
    uw = rnorm * (proj[nq:nq + docs] + proj[nq + docs:])
    factor = rnorm * (loss_scale / len_f)

    c_copy.wait_recv()
    rows_of = [spread[h * docs:(h + 1) * docs] for h in range(heads)]
    rows_of += [jnp.where(member, c_in[h:h + 1, :], 0.0) for h in range(heads)]
    for part in range(2):
        b_hi, b_lo = hi_lo(jnp.concatenate(rows_of[part::2], axis=0))
        a_ref[part] = jnp.concatenate([b_hi, b_lo], axis=0)

    qw_copy.wait_recv()
    qw = jnp.concatenate([qw_mine, qw_in[...]], axis=1)
    uw_copy.wait_recv()
    uw2 = factor * jnp.concatenate([uw, uw_in[...]], axis=1)
    factor = factor * sim_scale

    wait_all(stat.at[pl.ds(0, n_dp - 1)], s_recv)
    top = fold(
        n_dp, lambda k, c: jnp.maximum(c, stat[k][0:1]), jnp.full((1, nq), -jnp.inf, f32)
    )
    shifted = jnp.exp(logits - top)

    def gather(k, c):
        tile = stat[k]
        return c[0] + tile[1:2] * jnp.exp(tile[0:1] - top), c[1] + tile[2:3]

    zero = jnp.zeros((1, nq), f32)
    total, hit = fold(n_dp, gather, (zero, zero))
    dl = shifted * (1.0 / total) - chosen
    d_hi, d_lo = hi_lo(dl)
    g = mm(jnp.concatenate([d_hi, d_lo], axis=0), qw, NN)
    g = g[:docs] + g[docs:]
    inner = jnp.sum(dl * logits, axis=1, keepdims=True)
    loss_ref[0, 0] = jnp.sum(top + jnp.log(total) - hit) * (1.0 / nq)
    g = factor * g - inner * uw2
    tiles = [g[:, t * HD:(t + 1) * HD] for t in range(heads)]
    small = jnp.concatenate(tiles + tiles, axis=0).T.astype(bf16)
    out_ref[...] = (mm(small[:half], a_ref[0], NN) + mm(small[half:], a_ref[1], NN)).astype(bf16)

    wait_all(qall.at[pl.ds(0, peers)], send)
    pl.when(head == 0)(lambda: wait_all(emb_slot.at[0], send))
    pl.when(head > 0)(lambda: wait_all(emb_slot.at[pl.ds(0, n_head - 1)], send))
    wait_all(stat.at[pl.ds(0, n_dp - 1)], send)
    c_copy.wait_send()
    qw_copy.wait_send()
    uw_copy.wait_send()


def store(x_ref, l_ref, o_ref, lo_ref, sem):
    copies = [
        pltpu.make_async_copy(x_ref, o_ref, sem.at[0]),
        pltpu.make_async_copy(l_ref, lo_ref, sem.at[1]),
    ]
    for copy in copies:
        copy.start()
    for copy in copies:
        copy.wait()


def per_device(n_dp, n_head, attn_queries, keys, values, out_weight, lengths, queries, positives):
    seq, width = attn_queries.shape
    heads = width // HD
    docs = lengths.shape[1]
    rows = queries.shape[0]
    nq = n_dp * rows
    model = out_weight.shape[1]
    blocks = seq // LANES
    half = width // 2
    dma = pltpu.SemaphoreType.DMA
    hbm = pl.BlockSpec(memory_space=pltpu.HBM)
    vmem = pl.BlockSpec(memory_space=pltpu.VMEM)
    smem = pl.BlockSpec(memory_space=pltpu.SMEM)
    d_values, loss = pl.pallas_call(
        functools.partial(kernel, n_dp, n_head),
        out_shape=(
            pltpu.VMEM((HD // 2, seq), bf16),
            pltpu.SMEM((1, 1), f32),
        ),
        in_specs=[hbm, hbm, hbm, hbm, hbm, hbm, hbm],
        out_specs=(vmem, smem),
        scratch_shapes=[
            pltpu.SMEM((1, docs), jnp.int32),
            pltpu.VMEM((1, nq), jnp.int32),
            pltpu.VMEM((seq, width), bf16),
            pltpu.VMEM((seq, HD), bf16),
            pltpu.VMEM((seq, HD), bf16),
            pltpu.VMEM((width, model), bf16),
            pltpu.VMEM((n_dp * n_head, rows, width), bf16),
            pltpu.VMEM((nq, model), f32),
            pltpu.VMEM((SUBLANES // 2, seq), f32),
            pltpu.VMEM((SUBLANES // 2, seq), f32),
            pltpu.VMEM((n_head, docs, model), bf16),
            pltpu.VMEM((n_dp, SUBLANES // 2, nq), f32),
            pltpu.VMEM((nq, half), bf16),
            pltpu.VMEM((nq, half), bf16),
            pltpu.VMEM((docs, half), f32),
            pltpu.VMEM((docs, half), f32),
            pltpu.VMEM((2, 2 * heads * docs, seq), bf16),
            pltpu.VMEM((docs, model), bf16),
            pltpu.SemaphoreType.REGULAR((n_head,)),
            dma((6,)),
            dma,
            dma,
            dma,
            dma((2,)),
            dma,
            dma((3,)),
        ],
        compiler_params=pltpu.CompilerParams(collective_id=0, has_side_effects=True),
    )(lengths, positives.reshape(1, nq), attn_queries, keys, values, out_weight, queries)
    d_values = pltpu.with_memory_space_constraint(d_values, pltpu.VMEM)
    loss = pltpu.with_memory_space_constraint(loss, pltpu.SMEM)
    d_values, loss = pl.pallas_call(
        store,
        out_shape=(
            jax.ShapeDtypeStruct((HD // 2, seq), bf16),
            jax.ShapeDtypeStruct((1, 1), f32),
        ),
        in_specs=[vmem, smem],
        out_specs=(hbm, hbm),
        scratch_shapes=[dma((2,))],
    )(d_values, loss)
    return d_values.T, loss.reshape(())


def solution(mesh):
    placed = (
        P("dp", "head"),
        P("dp", None),
        P("dp", None),
        P("head", None),
        P("dp", None),
        P("dp", "head"),
        P(),
    )
    return jax.shard_map(
        functools.partial(per_device, mesh.shape["dp"], mesh.shape["head"]),
        mesh=mesh, in_specs=placed, out_specs=(P("dp", "head"), P()), check_vma=False,
    )
```
